32 devices in a mesh: grp: 2 (over y), hist: 4 (over z), chan: 2 (over x), seq: 2 (over core).
Axes of the slice: x: 2, y: 2, z: 4, core: 2. Of those that a mesh axis runs over, the one named last changes fastest.
Arguments:
- history: bfloat16 [16, 2048, 4096], P(('grp', 'seq'), 'hist', 'chan'), parts along dimension 0, may hold values from -6 to 6
- filter_taps: bfloat16 [4096, 4096], P(('grp', 'hist'), 'chan'), parts along dimension 0, may hold values from -0.125 to 0.125
- skip_gain: float32 [8192], P(('grp', 'chan')), parts along dimension 0, may hold values from -4 to 4
- gate_values: bfloat16 [16, 64, 4096], P(('grp', 'seq'), 'hist', 'chan'), parts along dimension 0, may hold values from -6 to 6
Outputs:
- output: bfloat16 [16, 64, 4096], P(('grp', 'seq'), 'hist', 'chan'), parts along dimension 0
The draws below stay inside these ranges and needn't reach their ends.
There are 2 independent parts, one for each index of `grp`. The reference program is written for one: setup_inputs(seed, part) draws one part's arguments, and reference() takes and returns one part's arrays. A program takes and returns all parts, laid end to end along the dimension named above; each array names one. Nothing has to cross between parts.
All inputs are finite; a program needn't handle non-finite values.
Results may differ from the reference program's by a relative error of at most 0.0085.
Values may be sent and summed in bfloat16 or wider, within the bound.
A program may use at most 192 MiB of HBM per device.

```python
import jax
import jax.numpy as jnp
from jax import lax

CH = 4096
SEQS = 8
NEW = 64
TOTAL = 2048


def steps_of(rng, dims, pieces, smallest, top_value):
    def one(axis_at, parts):
        steps = jax.random.uniform(jax.random.fold_in(jax.random.fold_in(rng, 6), axis_at), (parts,), jnp.float32, smallest / len(pieces), top_value / len(pieces))
        return jnp.repeat(jnp.exp(steps), dims[axis_at] // parts).reshape((-1,) + (1,) * (len(dims) - axis_at - 1))

    level = one(*pieces[0])
    for cut in pieces[1:]:
        level = level * one(*cut)
    return level


def scatter_about(rng, shape, spread, reach, pieces=(), dtype=jnp.bfloat16):
    loudness = steps_of(rng, shape, pieces, -0.22, 0.18) if pieces else 1.0
    values = jax.random.normal(rng, shape, jnp.float32) * spread * loudness
    return jnp.minimum(jnp.maximum(values, -reach), reach).astype(dtype)


def setup_inputs(seed: int = 0, part: int = 0) -> dict:
    arg_keys = jax.random.split(jax.random.key(seed), 5)
    part_keys = jax.random.split(jax.random.fold_in(arg_keys[4], part), 5)
    return {
        "history": scatter_about(part_keys[0], (SEQS, TOTAL, CH), 1.0, 6.0, ((0, 2), (1, 4), (2, 2))),
        "filter_taps": scatter_about(part_keys[1], (TOTAL, CH), TOTAL ** -0.5, 0.125, ((0, 4), (1, 2))),
        "skip_gain": scatter_about(part_keys[2], (CH,), 1.0, 4.0, ((0, 2),), jnp.float32),
        "gate_values": scatter_about(part_keys[3], (SEQS, NEW, CH), 1.0, 6.0, ((0, 2), (1, 4), (2, 2))),
    }


def reference(history, filter_taps, skip_gain, gate_values):
    full_len = history.shape[1]
    fft_len = 2 * full_len
    channels = history.shape[2]
    width = min(256, channels)
    blocks = channels // width
    inputs = history.reshape(history.shape[0], full_len, blocks, width).transpose(2, 0, 1, 3)
    filters = filter_taps[::-1].reshape(full_len, blocks, width).transpose(1, 0, 2)

    def per_block(pair):
        values, taps = pair
        spectrum_in = jnp.fft.rfft(values.astype(jnp.float32), n=fft_len, axis=1)
        spectrum_taps = jnp.fft.rfft(taps.astype(jnp.float32), n=fft_len, axis=0)
        result = jnp.fft.irfft(spectrum_in * spectrum_taps[None], n=fft_len, axis=1)
        return result[:, full_len - NEW:full_len].astype(jnp.float32)

    conv = lax.map(per_block, (inputs, filters))
    conv = conv.transpose(1, 2, 0, 3).reshape(history.shape[0], NEW, channels)
    newest = history[:, full_len - NEW:, :].astype(jnp.float32)
    mixed = conv + skip_gain[None, None, :] * newest
    return (gate_values.astype(jnp.float32) * mixed).astype(jnp.bfloat16)
```

```python
import functools
import math

import jax
import jax.numpy as jnp
import numpy as np
from jax import lax
from jax.experimental import pallas as pl
from jax.experimental.pallas import tpu as pltpu
from jax.sharding import PartitionSpec as P

MESH = pl.DeviceIdType.MESH
F32 = jnp.float32
BF16 = jnp.bfloat16
LAG = 2


def tables(new, piece):
    length = piece + new
    freqs = 2 * np.arange(length // 2)[:, None] + 1

    def both(times):
        angle = math.pi / length * (freqs * times[None, :] % (2 * length))
        return np.concatenate([np.cos(angle), np.sin(angle)], axis=0)

    taps_table = both(np.arange(length))
    data_table = both(np.arange(piece))
    back_table = both(new - 1 - np.arange(new)).T * (2.0 / length)
    return [jnp.asarray(table, BF16) for table in (taps_table, data_table, back_table)]


def kernel(
    n, new, piece, width, first,
    ft_hbm, fh_hbm, fi_hbm, hist_hbm, taps_hbm, gain_hbm, gate_hbm, out_hbm,
    ft, fh, fi, hist, taps, gain, gate, out, tspec, spec, part,
    send, recv, in_sem, small_sem, out_sem, rim_send, rim_recv, send_sem, recv_sem,
):
    me = lax.axis_index("hist")
    right, left = lax.rem(me + 1, n), lax.rem(me + n - 1, n)
    chunks, seqs, block, _ = hist.shape
    own = new // n
    half = n // 2
    bins = (piece + new) // 2
    pieces = block // piece

    def lanes(c):
        return pl.ds(pl.multiple_of(c * width, width), width)

    small = [
        pltpu.make_async_copy(source, target, small_sem.at[i])
        for i, (source, target) in enumerate(
            [(ft_hbm, ft), (fh_hbm, fh), (fi_hbm, fi), (gain_hbm, gain), (gate_hbm, gate)]
        )
    ]

    def load_taps(c):
        return pltpu.make_async_copy(
            taps_hbm.at[:, lanes(c)], taps.at[c, pl.ds(0, block)], in_sem.at[0, c]
        )

    def load_hist(c):
        return pltpu.make_async_copy(hist_hbm.at[:, :, lanes(c)], hist.at[c], in_sem.at[1, c])

    def store(c):
        return pltpu.make_async_copy(out.at[c], out_hbm.at[:, :, lanes(c)], out_sem.at[c])

    def rim_copy(c):
        return pltpu.make_async_remote_copy(
            src_ref=taps_hbm.at[pl.ds(0, new), lanes(c)],
            dst_ref=taps.at[c, pl.ds(block, new)],
            send_sem=rim_send.at[c],
            recv_sem=rim_recv.at[c],
            device_id={"hist": left},
            device_id_type=MESH,
        )

    def span(way, stage):
        if stage > 0:
            return 0, seqs
        return (0, first) if way == 0 else (first, seqs - first)

    def hop(way, stage, c):
        start, count = span(way, stage)
        return pltpu.make_async_remote_copy(
            src_ref=send.at[way, stage, c, pl.ds(start, count)],
            dst_ref=recv.at[way, stage, c, pl.ds(start, count)],
            send_sem=send_sem.at[way, stage, c],
            recv_sem=recv_sem.at[way, stage, c],
            device_id={"hist": right if way == 0 else left},
            device_id_type=MESH,
        )

    for copy in small[:3]:
        copy.start()

    def start_loads(c, carry):
        load_taps(c).start()
        load_hist(c).start()
        return carry

    lax.fori_loop(0, chunks, start_loads, 0)
    for copy in small[3:]:
        copy.start()

    barrier = pltpu.get_barrier_semaphore()
    for neighbour in (left, right):
        pl.semaphore_signal(barrier, inc=1, device_id={"hist": neighbour}, device_id_type=MESH)
    pl.semaphore_wait(barrier, 2)

    def start_rims(c, carry):
        rim_copy(c).start()
        return carry

    lax.fori_loop(0, chunks, start_rims, 0)
    for copy in small:
        copy.wait()
    last = (me == n - 1).astype(F32)
    inner = (me != n - 1).astype(F32)

    def compute(c):
        load_taps(c).wait()
        rim_copy(c).wait_recv()
        rim = taps[c, pl.ds(block, new)].astype(F32) * inner
        taps[c, pl.ds(block, new)] = rim.astype(BF16)
        for q in range(pieces):
            tspec[q] = jnp.dot(
                ft[...], taps[c, pl.ds(q * piece, piece + new)], preferred_element_type=F32
            )
        load_hist(c).wait()
        gains = gain[:, lanes(c)] * last
        for b in range(seqs):
            data = [
                jnp.dot(fh[...], hist[c, b, pl.ds(q * piece, piece)], preferred_element_type=F32)
                for q in range(pieces)
            ]
            for r in range(0, bins, 16):
                real = imag = None
                for q in range(pieces):
                    hc, hs = data[q][r : r + 16], data[q][bins + r : bins + r + 16]
                    tc, ts = tspec[q, pl.ds(r, 16)], tspec[q, pl.ds(bins + r, 16)]
                    one, two = tc * hc + ts * hs, ts * hc - tc * hs
                    real = one if q == 0 else real + one
                    imag = two if q == 0 else imag + two
                spec[b, pl.ds(r, 16)] = real.astype(BF16)
                spec[b, pl.ds(bins + r, 16)] = imag.astype(BF16)
            value = jnp.dot(fi[...], spec[b], preferred_element_type=F32)
            value = value + gains * hist[c, b, pl.ds(block - new, new)].astype(F32)
            for d in range(n):
                part[c, d, b] = value[d * own : (d + 1) * own]

    def pass_on(stage, c):
        for way in range(2):
            start, count = span(way, stage)
            if count == 0:
                continue
            ahead = half - stage
            owner = lax.rem(me + (ahead if way == 0 else n - ahead), n)
            before, size = span(way, stage - 1) if stage else (0, 0)
            if size:
                hop(way, stage - 1, c).wait_recv()
            for b in range(start, start + count):
                value = part[c, owner, b]
                if before <= b < before + size:
                    value = value + recv[way, stage - 1, c, b].astype(F32)
                send[way, stage, c, b] = value.astype(BF16)
            hop(way, stage, c).start()

    def finish(c):
        total = [part[c, me, b] for b in range(seqs)]
        for way in range(2):
            start, count = span(way, half - 1)
            if count == 0:
                continue
            hop(way, half - 1, c).wait_recv()
            for b in range(start, start + count):
                total[b] = total[b] + recv[way, half - 1, c, b].astype(F32)
        for b in range(seqs):
            out[c, b] = (gate[b, :, lanes(c)].astype(F32) * total[b]).astype(BF16)
        store(c).start()

    def step(i, carry):
        @pl.when(i < chunks)
        def _():
            compute(i)
            pass_on(0, i)

        for stage in range(1, half + 1):
            c = i - stage * LAG

            @pl.when(jnp.logical_and(c >= 0, c < chunks))
            def _():
                if stage < half:
                    pass_on(stage, c)
                else:
                    finish(c)

        return carry

    lax.fori_loop(0, chunks + half * LAG, step, 0)

    def drain(c, carry):
        store(c).wait()
        rim_copy(c).wait_send()
        for stage in range(half):
            for way in range(2):
                if span(way, stage)[1]:
                    hop(way, stage, c).wait_send()
        return carry

    lax.fori_loop(0, chunks, drain, 0)


def body(history, filter_taps, skip_gain, gate_values):
    n = lax.axis_size("hist")
    seqs, block, channels = history.shape
    own = gate_values.shape[1]
    new = own * n
    piece = min(2 * new, block)
    width = min(256, channels)
    chunks = channels // width
    half = n // 2
    length = piece + new
    first = (3 * seqs) // 4
    hbm = pl.BlockSpec(memory_space=pl.ANY)
    return pl.pallas_call(
        functools.partial(kernel, n, new, piece, width, first),
        out_shape=jax.ShapeDtypeStruct(gate_values.shape, BF16),
        in_specs=[hbm] * 7,
        out_specs=hbm,
        scratch_shapes=[
            pltpu.VMEM((length, length), BF16),
            pltpu.VMEM((length, piece), BF16),
            pltpu.VMEM((new, length), BF16),
            pltpu.VMEM((chunks, seqs, block, width), BF16),
            pltpu.VMEM((chunks, block + new, width), BF16),
            pltpu.VMEM((1, channels), F32),
            pltpu.VMEM(gate_values.shape, BF16),
            pltpu.VMEM((chunks, seqs, own, width), BF16),
            pltpu.VMEM((block // piece, length, width), F32),
            pltpu.VMEM((seqs, length, width), BF16),
            pltpu.VMEM((chunks, n, seqs, own, width), F32),
            pltpu.VMEM((2, half, chunks, seqs, own, width), BF16),
            pltpu.VMEM((2, half, chunks, seqs, own, width), BF16),
            pltpu.SemaphoreType.DMA((2, chunks)),
            pltpu.SemaphoreType.DMA((5,)),
            pltpu.SemaphoreType.DMA((chunks,)),
            pltpu.SemaphoreType.DMA((chunks,)),
            pltpu.SemaphoreType.DMA((chunks,)),
            pltpu.SemaphoreType.DMA((2, half, chunks)),
            pltpu.SemaphoreType.DMA((2, half, chunks)),
        ],
        compiler_params=pltpu.CompilerParams(
            collective_id=0, has_side_effects=True, vmem_limit_bytes=48 * 1024 * 1024
        ),
    )(*tables(new, piece), history, filter_taps, skip_gain[None, :], gate_values)


def solution(mesh):
    placed = (
        P(("grp", "seq"), "hist", "chan"),
        P(("grp", "hist"), "chan"),
        P(("grp", "chan")),
        P(("grp", "seq"), "hist", "chan"),
    )
    return jax.shard_map(
        body,
        mesh=mesh,
        in_specs=placed,
        out_specs=P(("grp", "seq"), "hist", "chan"),
        check_vma=False,
    )
```

```python
import functools
import math

import jax
import jax.numpy as jnp
import numpy as np
from jax import lax
from jax.experimental import pallas as pl
from jax.experimental.pallas import tpu as pltpu
from jax.sharding import PartitionSpec as P

MESH = pl.DeviceIdType.MESH
F32 = jnp.float32
BF16 = jnp.bfloat16
LAG = 2


def tables(new, piece):
    length = piece + new
    freqs = 2 * np.arange(length // 2)[:, None] + 1

    def both(times):
        angle = math.pi / length * (freqs * times[None, :] % (2 * length))
        return np.concatenate([np.cos(angle), np.sin(angle)], axis=0)

    taps_table = both(np.arange(length))
    data_table = both(np.arange(piece))
    back_table = both(new - 1 - np.arange(new)).T * (2.0 / length)
    return [jnp.asarray(table, BF16) for table in (taps_table, data_table, back_table)]


def kernel(
    n, new, piece, width, first,
    ft_hbm, fh_hbm, fi_hbm, hist_hbm, taps_hbm, gain_hbm, gate_hbm, out_hbm,
    ft, fh, fi, hist, taps, gain, gate, out, tspec, spec, part,
    send, recv, in_sem, small_sem, out_sem, rim_send, rim_recv, send_sem, recv_sem,
):
    me = lax.axis_index("hist")
    right, left = lax.rem(me + 1, n), lax.rem(me + n - 1, n)
    chunks, seqs, block, _ = hist.shape
    own = new // n
    half = n // 2
    bins = (piece + new) // 2
    pieces = block // piece

    def lanes(c):
        return pl.ds(pl.multiple_of(c * width, width), width)

    small = [
        pltpu.make_async_copy(source, target, small_sem.at[i])
        for i, (source, target) in enumerate(
            [(ft_hbm, ft), (fh_hbm, fh), (fi_hbm, fi), (gain_hbm, gain), (gate_hbm, gate)]
        )
    ]

    def load_taps(c):
        return pltpu.make_async_copy(
            taps_hbm.at[:, lanes(c)], taps.at[c, pl.ds(0, block)], in_sem.at[0, c]
        )

    def load_hist(c):
        return pltpu.make_async_copy(hist_hbm.at[:, :, lanes(c)], hist.at[c], in_sem.at[1, c])

    def store(c):
        return pltpu.make_async_copy(out.at[c], out_hbm.at[:, :, lanes(c)], out_sem.at[c])

    def rim_copy(c):
        return pltpu.make_async_remote_copy(
            src_ref=taps_hbm.at[pl.ds(0, new), lanes(c)],
            dst_ref=taps.at[c, pl.ds(block, new)],
            send_sem=rim_send.at[c],
            recv_sem=rim_recv.at[c],
            device_id={"hist": left},
            device_id_type=MESH,
        )

    def span(way, stage):
        if stage > 0:
            return 0, seqs
        return (0, first) if way == 0 else (first, seqs - first)

    def hop(way, stage, c):
        start, count = span(way, stage)
        return pltpu.make_async_remote_copy(
            src_ref=send.at[way, stage, c, pl.ds(start, count)],
            dst_ref=recv.at[way, stage, c, pl.ds(start, count)],
            send_sem=send_sem.at[way, stage, c],
            recv_sem=recv_sem.at[way, stage, c],
            device_id={"hist": right if way == 0 else left},
            device_id_type=MESH,
        )

    for copy in small[:3]:
        copy.start()

    def start_loads(c, carry):
        load_taps(c).start()
        load_hist(c).start()
        return carry

    lax.fori_loop(0, chunks, start_loads, 0)
    for copy in small[3:]:
        copy.start()

    barrier = pltpu.get_barrier_semaphore()
    for neighbour in (left, right):
        pl.semaphore_signal(barrier, inc=1, device_id={"hist": neighbour}, device_id_type=MESH)
    pl.semaphore_wait(barrier, 2)

    def start_rims(c, carry):
        rim_copy(c).start()
        return carry

    @pl.when(me != 0)
    def _():
        lax.fori_loop(0, chunks, start_rims, 0)

    for copy in small:
        copy.wait()
    last = (me == n - 1).astype(F32)

    def compute(c):
        load_taps(c).wait()

        @pl.when(me != n - 1)
        def _():
            rim_copy(c).wait_recv()

        @pl.when(me == n - 1)
        def _():
            taps[c, pl.ds(block, new)] = jnp.zeros((new, width), BF16)

        for q in range(pieces):
            tspec[q] = jnp.dot(
                ft[...], taps[c, pl.ds(q * piece, piece + new)], preferred_element_type=F32
            )
        load_hist(c).wait()
        gains = gain[:, lanes(c)] * last
        for b in range(seqs):
            data = [
                jnp.dot(fh[...], hist[c, b, pl.ds(q * piece, piece)], preferred_element_type=F32)
                for q in range(pieces)
            ]
            for r in range(0, bins, 16):
                real = imag = None
                for q in range(pieces):
                    hc, hs = data[q][r : r + 16], data[q][bins + r : bins + r + 16]
                    tc, ts = tspec[q, pl.ds(r, 16)], tspec[q, pl.ds(bins + r, 16)]
                    one, two = tc * hc + ts * hs, ts * hc - tc * hs
                    real = one if q == 0 else real + one
                    imag = two if q == 0 else imag + two
                spec[b, pl.ds(r, 16)] = real.astype(BF16)
                spec[b, pl.ds(bins + r, 16)] = imag.astype(BF16)
            value = jnp.dot(fi[...], spec[b], preferred_element_type=F32)
            value = value + gains * hist[c, b, pl.ds(block - new, new)].astype(F32)
            for d in range(n):
                part[c, d, b] = value[d * own : (d + 1) * own]

    def pass_on(stage, c):
        for way in range(2):
            start, count = span(way, stage)
            if count == 0:
                continue
            ahead = half - stage
            owner = lax.rem(me + (ahead if way == 0 else n - ahead), n)
            before, size = span(way, stage - 1) if stage else (0, 0)
            if size:
                hop(way, stage - 1, c).wait_recv()
            for b in range(start, start + count):
                value = part[c, owner, b]
                if before <= b < before + size:
                    value = value + recv[way, stage - 1, c, b].astype(F32)
                send[way, stage, c, b] = value.astype(BF16)
            hop(way, stage, c).start()

    def finish(c):
        total = [part[c, me, b] for b in range(seqs)]
        for way in range(2):
            start, count = span(way, half - 1)
            if count == 0:
                continue
            hop(way, half - 1, c).wait_recv()
            for b in range(start, start + count):
                total[b] = total[b] + recv[way, half - 1, c, b].astype(F32)
        for b in range(seqs):
            out[c, b] = (gate[b, :, lanes(c)].astype(F32) * total[b]).astype(BF16)
        store(c).start()

    def step(i, carry):
        @pl.when(i < chunks)
        def _():
            compute(i)
            pass_on(0, i)

        for stage in range(1, half + 1):
            c = i - stage * LAG

            @pl.when(jnp.logical_and(c >= 0, c < chunks))
            def _():
                if stage < half:
                    pass_on(stage, c)
                else:
                    finish(c)

        return carry

    lax.fori_loop(0, chunks + half * LAG, step, 0)

    def drain(c, carry):
        store(c).wait()

        @pl.when(me != 0)
        def _():
            rim_copy(c).wait_send()

        for stage in range(half):
            for way in range(2):
                if span(way, stage)[1]:
                    hop(way, stage, c).wait_send()
        return carry

    lax.fori_loop(0, chunks, drain, 0)


def body(history, filter_taps, skip_gain, gate_values):
    n = lax.axis_size("hist")
    seqs, block, channels = history.shape
    own = gate_values.shape[1]
    new = own * n
    piece = min(2 * new, block)
    width = min(256, channels)
    chunks = channels // width
    half = n // 2
    length = piece + new
    first = (3 * seqs) // 4
    hbm = pl.BlockSpec(memory_space=pl.ANY)
    return pl.pallas_call(
        functools.partial(kernel, n, new, piece, width, first),
        out_shape=jax.ShapeDtypeStruct(gate_values.shape, BF16),
        in_specs=[hbm] * 7,
        out_specs=hbm,
        scratch_shapes=[
            pltpu.VMEM((length, length), BF16),
            pltpu.VMEM((length, piece), BF16),
            pltpu.VMEM((new, length), BF16),
            pltpu.VMEM((chunks, seqs, block, width), BF16),
            pltpu.VMEM((chunks, block + new, width), BF16),
            pltpu.VMEM((1, channels), F32),
            pltpu.VMEM(gate_values.shape, BF16),
            pltpu.VMEM((chunks, seqs, own, width), BF16),
            pltpu.VMEM((block // piece, length, width), F32),
            pltpu.VMEM((seqs, length, width), BF16),
            pltpu.VMEM((chunks, n, seqs, own, width), F32),
            pltpu.VMEM((2, half, chunks, seqs, own, width), BF16),
            pltpu.VMEM((2, half, chunks, seqs, own, width), BF16),
            pltpu.SemaphoreType.DMA((2, chunks)),
            pltpu.SemaphoreType.DMA((5,)),
            pltpu.SemaphoreType.DMA((chunks,)),
            pltpu.SemaphoreType.DMA((chunks,)),
            pltpu.SemaphoreType.DMA((chunks,)),
            pltpu.SemaphoreType.DMA((2, half, chunks)),
            pltpu.SemaphoreType.DMA((2, half, chunks)),
        ],
        compiler_params=pltpu.CompilerParams(
            collective_id=0, has_side_effects=True, vmem_limit_bytes=60 * 1024 * 1024
        ),
    )(*tables(new, piece), history, filter_taps, skip_gain[None, :], gate_values)


def solution(mesh):
    placed = (
        P(("grp", "seq"), "hist", "chan"),
        P(("grp", "hist"), "chan"),
        P(("grp", "chan")),
        P(("grp", "seq"), "hist", "chan"),
    )
    return jax.shard_map(
        body,
        mesh=mesh,
        in_specs=placed,
        out_specs=P(("grp", "seq"), "hist", "chan"),
        check_vma=False,
    )
```

```python
import functools
import math

import jax
import jax.numpy as jnp
import numpy as np
from jax import lax
from jax.experimental import pallas as pl
from jax.experimental.pallas import tpu as pltpu
from jax.sharding import PartitionSpec as P

MESH = pl.DeviceIdType.MESH
F32 = jnp.float32
BF16 = jnp.bfloat16
LAG = 3


def tables(new, piece):
    length = piece + new
    freqs = 2 * np.arange(length // 2)[:, None] + 1

    def both(times):
        angle = math.pi / length * (freqs * times[None, :] % (2 * length))
        return np.concatenate([np.cos(angle), np.sin(angle)], axis=0)

    taps_table = both(np.arange(length))
    data_table = both(np.arange(piece))
    back_table = both(new - 1 - np.arange(new)).T * (2.0 / length)
    return [jnp.asarray(table, BF16) for table in (taps_table, data_table, back_table)]


def kernel(
    n, new, piece, width, first,
    ft_hbm, fh_hbm, fi_hbm, hist_hbm, taps_hbm, gain_hbm, gate_hbm, out_hbm,
    ft, fh, fi, hist, taps, gain, gate, out, tspec, spec, part,
    send, recv, in_sem, small_sem, out_sem, rim_send, rim_recv, send_sem, recv_sem,
):
    me = lax.axis_index("hist")
    right, left = lax.rem(me + 1, n), lax.rem(me + n - 1, n)
    chunks, seqs, block, _ = hist.shape
    own = new // n
    half = n // 2
    bins = (piece + new) // 2
    pieces = block // piece

    def lanes(c):
        return pl.ds(pl.multiple_of(c * width, width), width)

    small = [
        pltpu.make_async_copy(source, target, small_sem.at[i])
        for i, (source, target) in enumerate(
            [(ft_hbm, ft), (fh_hbm, fh), (fi_hbm, fi), (gain_hbm, gain), (gate_hbm, gate)]
        )
    ]

    def load_taps(c):
        return pltpu.make_async_copy(
            taps_hbm.at[:, lanes(c)], taps.at[c, pl.ds(0, block)], in_sem.at[0, c]
        )

    def load_hist(c):
        return pltpu.make_async_copy(hist_hbm.at[:, :, lanes(c)], hist.at[c], in_sem.at[1, c])

    def store(c):
        return pltpu.make_async_copy(out.at[c], out_hbm.at[:, :, lanes(c)], out_sem.at[c])

    def rim_copy(c):
        return pltpu.make_async_remote_copy(
            src_ref=taps_hbm.at[pl.ds(0, new), lanes(c)],
            dst_ref=taps.at[c, pl.ds(block, new)],
            send_sem=rim_send.at[c],
            recv_sem=rim_recv.at[c],
            device_id={"hist": left},
            device_id_type=MESH,
        )

    def span(way, stage):
        if stage > 0:
            return 0, seqs
        return (0, first) if way == 0 else (first, seqs - first)

    def hop(way, stage, c):
        start, count = span(way, stage)
        return pltpu.make_async_remote_copy(
            src_ref=send.at[way, stage, c, pl.ds(start, count)],
            dst_ref=recv.at[way, stage, c, pl.ds(start, count)],
            send_sem=send_sem.at[way, stage, c],
            recv_sem=recv_sem.at[way, stage, c],
            device_id={"hist": right if way == 0 else left},
            device_id_type=MESH,
        )

    for copy in small[:3]:
        copy.start()

    def start_loads(c, carry):
        load_taps(c).start()
        load_hist(c).start()
        return carry

    lax.fori_loop(0, chunks, start_loads, 0)
    for copy in small[3:]:
        copy.start()

    barrier = pltpu.get_barrier_semaphore()
    for neighbour in (left, right):
        pl.semaphore_signal(barrier, inc=1, device_id={"hist": neighbour}, device_id_type=MESH)
    pl.semaphore_wait(barrier, 2)

    def start_rims(c, carry):
        rim_copy(c).start()
        return carry

    @pl.when(me != 0)
    def _():
        lax.fori_loop(0, chunks, start_rims, 0)

    for copy in small:
        copy.wait()
    last = (me == n - 1).astype(F32)

    def compute(c):
        load_taps(c).wait()

        @pl.when(me != n - 1)
        def _():
            rim_copy(c).wait_recv()

        @pl.when(me == n - 1)
        def _():
            taps[c, pl.ds(block, new)] = jnp.zeros((new, width), BF16)

        for q in range(pieces):
            tspec[q] = jnp.dot(
                ft[...], taps[c, pl.ds(q * piece, piece + new)], preferred_element_type=F32
            )
        load_hist(c).wait()
        gains = gain[:, lanes(c)] * last
        for b in range(seqs):
            data = [
                jnp.dot(fh[...], hist[c, b, pl.ds(q * piece, piece)], preferred_element_type=F32)
                for q in range(pieces)
            ]
            for r in range(0, bins, 16):
                real = imag = None
                for q in range(pieces):
                    hc, hs = data[q][r : r + 16], data[q][bins + r : bins + r + 16]
                    tc, ts = tspec[q, pl.ds(r, 16)], tspec[q, pl.ds(bins + r, 16)]
                    one, two = tc * hc + ts * hs, ts * hc - tc * hs
                    real = one if q == 0 else real + one
                    imag = two if q == 0 else imag + two
                spec[b, pl.ds(r, 16)] = real.astype(BF16)
                spec[b, pl.ds(bins + r, 16)] = imag.astype(BF16)
            value = jnp.dot(fi[...], spec[b], preferred_element_type=F32)
            value = value + gains * hist[c, b, pl.ds(block - new, new)].astype(F32)
            for d in range(n):
                part[c, d, b] = value[d * own : (d + 1) * own]

    def pass_on(stage, c):
        for way in range(2):
            start, count = span(way, stage)
            if count == 0:
                continue
            ahead = half - stage
            owner = lax.rem(me + (ahead if way == 0 else n - ahead), n)
            before, size = span(way, stage - 1) if stage else (0, 0)
            if size:
                hop(way, stage - 1, c).wait_recv()
            for b in range(start, start + count):
                value = part[c, owner, b]
                if before <= b < before + size:
                    value = value + recv[way, stage - 1, c, b].astype(F32)
                send[way, stage, c, b] = value.astype(BF16)
            hop(way, stage, c).start()

    def finish(c):
        total = [part[c, me, b] for b in range(seqs)]
        for way in range(2):
            start, count = span(way, half - 1)
            if count == 0:
                continue
            hop(way, half - 1, c).wait_recv()
            for b in range(start, start + count):
                total[b] = total[b] + recv[way, half - 1, c, b].astype(F32)
        for b in range(seqs):
            out[c, b] = (gate[b, :, lanes(c)].astype(F32) * total[b]).astype(BF16)
        store(c).start()

    def step(i, carry):
        @pl.when(i < chunks)
        def _():
            compute(i)
            pass_on(0, i)

        for stage in range(1, half + 1):
            c = i - stage * LAG

            @pl.when(jnp.logical_and(c >= 0, c < chunks))
            def _():
                if stage < half:
                    pass_on(stage, c)
                else:
                    finish(c)

        return carry

    lax.fori_loop(0, chunks + half * LAG, step, 0)

    def drain(c, carry):
        store(c).wait()

        @pl.when(me != 0)
        def _():
            rim_copy(c).wait_send()

        for stage in range(half):
            for way in range(2):
                if span(way, stage)[1]:
                    hop(way, stage, c).wait_send()
        return carry

    lax.fori_loop(0, chunks, drain, 0)


def body(history, filter_taps, skip_gain, gate_values):
    n = lax.axis_size("hist")
    seqs, block, channels = history.shape
    own = gate_values.shape[1]
    new = own * n
    piece = min(2 * new, block)
    width = min(256, channels)
    chunks = channels // width
    half = n // 2
    length = piece + new
    first = (3 * seqs) // 4
    hbm = pl.BlockSpec(memory_space=pl.ANY)
    return pl.pallas_call(
        functools.partial(kernel, n, new, piece, width, first),
        out_shape=jax.ShapeDtypeStruct(gate_values.shape, BF16),
        in_specs=[hbm] * 7,
        out_specs=hbm,
        scratch_shapes=[
            pltpu.VMEM((length, length), BF16),
            pltpu.VMEM((length, piece), BF16),
            pltpu.VMEM((new, length), BF16),
            pltpu.VMEM((chunks, seqs, block, width), BF16),
            pltpu.VMEM((chunks, block + new, width), BF16),
            pltpu.VMEM((1, channels), F32),
            pltpu.VMEM(gate_values.shape, BF16),
            pltpu.VMEM((chunks, seqs, own, width), BF16),
            pltpu.VMEM((block // piece, length, width), F32),
            pltpu.VMEM((seqs, length, width), BF16),
            pltpu.VMEM((chunks, n, seqs, own, width), F32),
            pltpu.VMEM((2, half, chunks, seqs, own, width), BF16),
            pltpu.VMEM((2, half, chunks, seqs, own, width), BF16),
            pltpu.SemaphoreType.DMA((2, chunks)),
            pltpu.SemaphoreType.DMA((5,)),
            pltpu.SemaphoreType.DMA((chunks,)),
            pltpu.SemaphoreType.DMA((chunks,)),
            pltpu.SemaphoreType.DMA((chunks,)),
            pltpu.SemaphoreType.DMA((2, half, chunks)),
            pltpu.SemaphoreType.DMA((2, half, chunks)),
        ],
        compiler_params=pltpu.CompilerParams(
            collective_id=0, has_side_effects=True, vmem_limit_bytes=60 * 1024 * 1024
        ),
    )(*tables(new, piece), history, filter_taps, skip_gain[None, :], gate_values)


def solution(mesh):
    placed = (
        P(("grp", "seq"), "hist", "chan"),
        P(("grp", "hist"), "chan"),
        P(("grp", "chan")),
        P(("grp", "seq"), "hist", "chan"),
    )
    return jax.shard_map(
        body,
        mesh=mesh,
        in_specs=placed,
        out_specs=P(("grp", "seq"), "hist", "chan"),
        check_vma=False,
    )
```
